32 devices in a mesh: dp: 32 (over z, y, x, core), tensor: 1.
Axes of the slice: x: 2, y: 2, z: 4, core: 2. Of those that a mesh axis runs over, the one named last changes fastest.
Arguments:
- master: float32 [3, 4, 1024, 2048], P(None, None, 'dp', 'tensor'), may hold values from -6 to 6
- moment_one: float32 [3, 4, 1024, 2048], P(None, None, 'dp', 'tensor'), may hold values from -4 to 4
- moment_two: float32 [3, 4, 1024, 2048], P(None, None, 'dp', 'tensor'), may hold values from 0.01 to 1
- gradients: bfloat16 [3, 4, 1024, 2048], P(None, None, 'dp', 'tensor'), may hold values from -10000 to 10000
- norm_gain: float32 [2048], replicated, may hold values from 0.1 to 1.9
- hidden_in: bfloat16 [4, 128, 2048], P(None, ('dp', 'tensor')), may hold values from -6 to 6
- expert_ids: int32 [4, 128, 2], P(None, ('dp', 'tensor')), may hold values from 0 to 3, all different within a row; in each aligned block of 4 rows (0 to 3, 4 to 7, ..., all dimensions but the last counted through in order) at most 4 rows name the same one
- route_weights: float32 [4, 128, 2], P(None, ('dp', 'tensor')), may hold values from 0.05 to 1
Outputs:
- new_master: float32 [3, 4, 1024, 2048], P(None, None, 'dp', 'tensor')
- new_moment_one: float32 [3, 4, 1024, 2048], P(None, None, 'dp', 'tensor')
- new_moment_two: float32 [3, 4, 1024, 2048], P(None, None, 'dp', 'tensor')
- served_weights: bfloat16 [3, 4096, 2048], P(None, 'dp')
- decoded: bfloat16 [4, 128, 2048], P(None, ('dp', 'tensor'))
The draws below stay inside these ranges and needn't reach their ends.
Inputs may be any that keep to these rules, and one draw needn't show every extreme that they name: `expert_ids`: A row names 2 different experts; in each step the 4 rows of one device name one expert at most 4 times.
All inputs are finite; a program needn't handle non-finite values.
Results may differ from the reference program's by a relative error of at most 0.0067.
Values may be sent and summed in bfloat16 or wider, within the bound.
No kernel may reach another device: no remote copies, remote signals or barrier semaphores. Data moves between devices by JAX's collectives and lax.ppermute only.
A program may use at most 64 MiB of HBM per device.

```python
import math
import jax
import jax.numpy as jnp
import numpy as np
from jax import lax

D = 2048
FF = 1024
FF_DEV = 128
TOP = 2
STEPS = 4
ROWS_DEV = 4
GROUP = 8
EXPERTS = 4
STRIP = 4
CAP = 4
TOKENS = 128
COUNT = 25165824
N_DP = 32


def draw_gradients(key, part):
    subkeys = jax.random.split(jax.random.fold_in(key, 7), 3)
    full_shape = (3, EXPERTS, FF, D)
    random_part = jnp.clip(jax.random.normal(subkeys[0], full_shape, jnp.float32), -5.0, 5.0)
    row_scale = jnp.exp(jax.random.uniform(subkeys[1], (3, EXPERTS, FF, 1), jnp.float32) * math.log(10.0))
    column_scale = jnp.exp(jax.random.uniform(subkeys[2], (D,), jnp.float32) * math.log(10.0))
    unit_ramp = jnp.exp(0.5 * math.log(3.0) * jnp.arange(FF, dtype=jnp.float32) / FF)
    width_ramp = jnp.exp(0.5 * math.log(3.0) * jnp.arange(D, dtype=jnp.float32) / D)
    values = random_part * row_scale * column_scale * unit_ramp[:, None] * width_ramp
    return values.astype(jnp.bfloat16)


def levels(key, extent, shards, smallest, top_value):
    def one(position, blocks):
        draws = jax.random.uniform(jax.random.fold_in(jax.random.fold_in(key, 6), position), (blocks,), jnp.float32, smallest / len(shards), top_value / len(shards))
        return jnp.repeat(jnp.exp(draws), extent[position] // blocks).reshape((-1,) + (1,) * (len(extent) - position - 1))

    level = one(*shards[0])
    for cut in shards[1:]:
        level = level * one(*cut)
    return level


def shared_out(rng, own, number, rows, count, top, bound, skew):
    ranking = jax.random.permutation(rng, count)
    crowded, usual = load_shares(count, rows * top, bound, skew, True), load_shares(count, rows * top, bound, skew, False)
    places = jnp.arange(count)

    def named(tallies, offset_by):
        used = int((tallies > 0).sum())
        fixed = max(1, used // 4)
        moved = fixed + (places - fixed + offset_by * (used - fixed)) % max(1, count - fixed)
        return jnp.zeros((count,), jnp.int32).at[ranking[jnp.where(places < fixed, places, moved)]].set(jnp.asarray(tallies, jnp.int32))

    tallies = jnp.where(number % 4 == 0, named(crowded, number // 4), named(usual, number - number // 4 - 1))
    mixed = jax.random.permutation(jax.random.fold_in(own, 3), count)
    donor, receiver = mixed[0:count // 2 * 2:2], mixed[1:count // 2 * 2:2]
    slack = jnp.minimum(tallies[donor] - 1, bound - tallies[receiver]) // 2
    slack = jnp.where((donor == ranking[0]) | (receiver == ranking[0]) | (tallies[receiver] == 0), 0, jnp.maximum(slack, 0))
    moved = jax.random.randint(jax.random.fold_in(own, 4), (count // 2,), 0, 1 << 20) % (slack + 1)
    tallies = tallies.at[donor].add(-moved).at[receiver].add(moved)
    members = jnp.searchsorted(jnp.cumsum(tallies), jnp.arange(rows * top), side="right").astype(jnp.int32)
    listing = members.reshape(top, rows).T
    listing = listing[jax.random.permutation(jax.random.fold_in(own, 1), rows)]
    offset_by = jax.random.randint(jax.random.fold_in(own, 2), (rows, 1), 0, top)
    return jnp.take_along_axis(listing, (jnp.arange(top)[None, :] + offset_by) % top, axis=1)


def load_shares(count, total, most, slope, full):
    weights = [(1 << 20) // math.isqrt(rank ** slope) + 1 for rank in range(1, count + 1)]
    largest = most if full else min(most, max(-(-total // count), total * weights[0] // sum(weights)))
    least = 1 if total - largest >= count - 1 else 0
    holding, rest = [largest] + [least] * (count - 1), total - largest - least * (count - 1)
    while rest > 0:
        movable = [i for i in range(1, count) if holding[i] < largest] or [i for i in range(1, count) if holding[i] < most]
        pool, left = sum([weights[i] for i in movable]), rest
        for i in movable:
            extra = min(most - holding[i], max(1, left * weights[i] // pool), rest)
            holding[i] = holding[i] + extra
            rest = rest - extra
    return np.array(holding)


def normal_values(own_key, shape, width, most, shards=(), kind=jnp.bfloat16):
    drawn = jax.random.normal(own_key, shape, jnp.float32) * width
    if len(shards) > 0:
        drawn = levels(own_key, shape, shards, -0.22, 0.18) * drawn
    return jnp.clip(drawn, min=-most, max=most).astype(kind)


def setup_inputs(seed: int = 0) -> dict:
    key_of = jax.random.split(jax.random.key(seed), 9)
    master = normal_values(key_of[0], (3, EXPERTS, FF, D), 1.0, 6.0, ((2, 32),), jnp.float32)
    moment_one = normal_values(key_of[1], (3, EXPERTS, FF, D), 0.3, 4.0, ((2, 32),), jnp.float32)
    moment_two = jnp.clip(jnp.exp(math.log(1.0) - 4.6051702 * jax.random.uniform(key_of[2], (3, EXPERTS, FF, D), jnp.float32) ** levels(key_of[2], (3, EXPERTS, FF, D), ((2, 32),), -0.2, 0.2)), 0.01, 1.0)
    gradients = draw_gradients(jax.random.fold_in(key_of[8], 71), 0)
    norm_gain = jnp.clip(1.0 + 0.18 * jax.random.normal(key_of[4], (D,), jnp.float32), 0.1, 1.9)
    hidden_in = normal_values(key_of[5], (STEPS, TOKENS, D), 1.0, 6.0, ((1, 32),))
    expert_ids_keys = jax.random.split(jax.random.fold_in(key_of[6], 1), STEPS * TOKENS // ROWS_DEV)
    expert_ids_turns = jax.random.permutation(jax.random.fold_in(key_of[6], 3), STEPS * TOKENS // ROWS_DEV)
    expert_ids = jax.vmap(lambda own, number: shared_out(jax.random.fold_in(key_of[6], 2), own, number, ROWS_DEV, EXPERTS, TOP, CAP, 1))(expert_ids_keys, expert_ids_turns).reshape((STEPS, TOKENS, TOP))
    route_weights = jnp.clip(jnp.exp(math.log(1.0) - 2.9957323 * jax.random.uniform(key_of[7], (STEPS, TOKENS, TOP), jnp.float32) ** levels(key_of[7], (STEPS, TOKENS, TOP), ((1, 32),), -0.2, 0.2)), 0.05, 1.0)
    return {"master": master, "moment_one": moment_one, "moment_two": moment_two, "gradients": gradients, "norm_gain": norm_gain, "hidden_in": hidden_in, "expert_ids": expert_ids, "route_weights": route_weights}


beta_one = 0.9
beta_two = 0.95
learn_rate = 0.02
decay_rate = 0.1
adam_eps = 1e-08
step_count = 10
norm_eps = 1e-06

def adam_update(master, moment_one, moment_two, gradients, clip_factor):
    scaled = gradients.astype(jnp.float32) * clip_factor
    first_moment = beta_one * moment_one + (1.0 - beta_one) * scaled
    second = beta_two * moment_two + (1.0 - beta_two) * scaled * scaled
    first_fix = 1.0 - beta_one ** step_count
    second_fix = 1.0 - beta_two ** step_count
    update = first_moment / first_fix / (jnp.sqrt(second / second_fix) + adam_eps)
    return (master - learn_rate * (update + decay_rate * master), first_moment, second)

def decode_step(token_rows, step_ids, step_gates, into_weights, down_weights, norm_gain):
    widened = token_rows.astype(jnp.float32)
    factor = lax.rsqrt(lax.optimization_barrier(jnp.mean(widened * widened, axis=1, keepdims=True)) + norm_eps)
    normed = (widened * factor * norm_gain).astype(jnp.bfloat16)
    shares = step_gates / lax.optimization_barrier(jnp.sum(step_gates, axis=1, keepdims=True))
    pair_keys = step_ids.reshape(-1).astype(jnp.int32)
    pair_order = jnp.argsort(pair_keys, stable=True).astype(jnp.int32)
    owner_row = pair_order // TOP
    picked = normed[owner_row]
    counts = lax.optimization_barrier(jnp.sum((pair_keys[:, None] == jnp.arange(EXPERTS, dtype=jnp.int32)[None, :]).astype(jnp.int32), axis=0)).astype(jnp.int32)
    projected = lax.ragged_dot(picked, into_weights, counts, preferred_element_type=jnp.float32) / math.sqrt(D)
    active = (jax.nn.silu(projected[:, :FF]) * projected[:, FF:]).astype(jnp.bfloat16)
    summed = jnp.zeros((pair_keys.shape[0], D), jnp.float32)
    for group_index in range(GROUP):
        lower = group_index * FF_DEV
        group_part = lax.ragged_dot(active[:, lower:lower + FF_DEV], down_weights[:, lower:lower + FF_DEV, :], counts, preferred_element_type=jnp.float32)
        rounded = (group_part / math.sqrt(FF)).astype(jnp.bfloat16)
        rounded = lax.optimization_barrier(rounded)
        summed = summed + rounded.astype(jnp.float32)
    weight = shares.reshape(-1)[pair_order]
    result = widened.at[owner_row].add(weight[:, None] * summed)
    return result.astype(jnp.bfloat16)

def reference(master, moment_one, moment_two, gradients, norm_gain, hidden_in, expert_ids, route_weights):
    widened = gradients.astype(jnp.float32)
    squares = jnp.sum(widened * widened)
    clip_factor = jnp.minimum(1.0, lax.rsqrt(squares / COUNT + norm_eps))
    new_master, new_one, new_two = adam_update(master, moment_one, moment_two, gradients, clip_factor)
    rounded = new_master.astype(jnp.bfloat16)
    regrouped = rounded.reshape(3, EXPERTS, N_DP, GROUP, STRIP, D)
    served = jnp.transpose(regrouped, (0, 1, 3, 2, 4, 5)).reshape(3, EXPERTS * FF, D)
    weights = served.reshape(3, EXPERTS, FF, D)
    into_weights = jnp.swapaxes(jnp.concatenate([weights[0], weights[1]], axis=1), 1, 2)
    decoded_steps = []
    for step_index in range(STEPS):
        decoded_steps.append(decode_step(hidden_in[step_index], expert_ids[step_index], route_weights[step_index], into_weights, weights[2], norm_gain))
    return (new_master, new_one, new_two, served, jnp.stack(decoded_steps))
```

```python
import math

import jax
import jax.numpy as jnp
from jax import lax
from jax.sharding import PartitionSpec as P


beta_one = 0.9
beta_two = 0.95
learn_rate = 0.02
decay_rate = 0.1
adam_eps = 1e-08
step_count = 10
norm_eps = 1e-06
lanes = 128


def adam_update(master, moment_one, moment_two, gradients, clip_factor):
    scaled = gradients.astype(jnp.float32) * clip_factor
    first_moment = beta_one * moment_one + (1.0 - beta_one) * scaled
    second = beta_two * moment_two + (1.0 - beta_two) * scaled * scaled
    first_fix = 1.0 - beta_one**step_count
    second_fix = 1.0 - beta_two**step_count
    update = first_moment / first_fix / (jnp.sqrt(second / second_fix) + adam_eps)
    return (master - learn_rate * (update + decay_rate * master), first_moment, second)


def exchange(value, offset, member_count):
    return lax.ppermute(value, "dp", [(i, i ^ offset) for i in range(member_count)])


def stage_offsets(member_count):
    bits = member_count.bit_length() - 1
    assert 1 << bits == member_count
    pair = bits % 2
    stages = [[k << b for k in range(4)] for b in range(pair, bits, 2)]
    return (1 if pair else 0, stages)


def per_device(
    master, moment_one, moment_two, gradients, norm_gain, hidden_in, expert_ids, route_weights
):
    slice_count = lax.axis_size("tensor")
    member_count = lax.axis_size("dp")
    expert_count = master.shape[1]
    local_units = master.shape[2]
    local_width = master.shape[3]
    hidden_total = local_units * member_count
    model_width = local_width * slice_count
    entries = 3 * expert_count * hidden_total * model_width
    pair, stages = stage_offsets(member_count)

    widened = gradients.astype(jnp.float32)
    partial_sum = jnp.sum(widened * widened)
    sums = lax.all_to_all(
        jnp.broadcast_to(partial_sum, (member_count, lanes)),
        "dp",
        split_axis=0,
        concat_axis=0,
        tiled=True,
    )
    squares = jnp.sum(sums[:, 0])
    if slice_count > 1:
        squares = lax.psum(squares, "tensor")
    clip_factor = jnp.minimum(1.0, lax.rsqrt(squares / entries + norm_eps))

    step_total, row_count = hidden_in.shape[:2]
    rows = hidden_in.reshape(step_total * row_count, model_width).astype(jnp.float32)
    factor = lax.rsqrt(jnp.mean(rows * rows, axis=1, keepdims=True) + norm_eps)
    normed = (rows * factor * norm_gain).astype(jnp.bfloat16)
    gates = route_weights.reshape(step_total * row_count, -1)
    shares = gates / jnp.sum(gates, axis=1, keepdims=True)
    ids = expert_ids.reshape(step_total * row_count, -1)
    expert_lane = jnp.arange(lanes, dtype=jnp.int32)
    combine = jnp.sum(
        jnp.where(ids[:, :, None] == expert_lane[None, None, :], shares[:, :, None], 0.0), axis=1
    )
    high = combine.astype(jnp.bfloat16)
    low = (combine - high.astype(jnp.float32)).astype(jnp.bfloat16)
    gathered = jnp.concatenate([normed, high, low], axis=1)[None]
    for offsets in reversed(stages):
        gathered = jnp.stack(
            [gathered] + [exchange(gathered, k, member_count) for k in offsets[1:]]
        ).reshape((-1,) + gathered.shape[1:])

    new_master, new_one, new_two = adam_update(
        master, moment_one, moment_two, gradients, clip_factor
    )
    rounded = new_master.astype(jnp.bfloat16)
    whole = rounded
    if slice_count > 1:
        whole = lax.all_gather(rounded, "tensor", axis=3, tiled=True)

    group_size = member_count // expert_count
    strip_width = local_units // group_size
    ordered = whole.reshape(3, member_count, strip_width, model_width).transpose(1, 0, 2, 3)
    owned = lax.all_to_all(ordered, "dp", split_axis=0, concat_axis=0, tiled=True)
    served = owned.transpose(1, 0, 2, 3).reshape(3, member_count * strip_width, model_width)

    weights = whole.reshape(3, 1, expert_count * local_units, model_width)
    if pair:
        weights = jnp.concatenate([weights, exchange(weights, pair, member_count)], axis=1)
    weights = weights.reshape(3, -1, model_width)
    token_rows = gathered.reshape(-1, gathered.shape[-1])
    inputs = token_rows[:, :model_width]
    mix = token_rows[:, model_width : model_width + expert_count].astype(jnp.float32) + token_rows[
        :, model_width + lanes : model_width + lanes + expert_count
    ].astype(jnp.float32)
    contract = (((1,), (1,)), ((), ()))
    gate = lax.dot_general(inputs, weights[0], contract, preferred_element_type=jnp.float32)
    up = lax.dot_general(inputs, weights[1], contract, preferred_element_type=jnp.float32)
    scale = 1.0 / math.sqrt(model_width)
    active = jax.nn.silu(gate * scale) * (up * scale)
    total_rows = active.shape[0]
    active = active.reshape(total_rows, -1, expert_count, local_units) * mix[:, None, :, None]
    active = active.reshape(total_rows, -1).astype(jnp.bfloat16)
    partial_out = jnp.dot(active, weights[2], preferred_element_type=jnp.float32) / math.sqrt(
        hidden_total
    )
    summed = partial_out.reshape(gathered.shape[:2] + (model_width,))

    for offsets in stages:
        parts = summed.reshape((len(offsets), -1) + summed.shape[1:])
        sent = parts.astype(jnp.bfloat16)
        summed = parts[0]
        for index, k in enumerate(offsets[1:], 1):
            summed = summed + exchange(sent[index], k, member_count).astype(jnp.float32)
    decoded = (rows + summed[0]).astype(jnp.bfloat16).reshape(hidden_in.shape)
    return (new_master, new_one, new_two, served, decoded)


def solution(mesh):
    in_specs = (
        P(None, None, "dp", "tensor"),
        P(None, None, "dp", "tensor"),
        P(None, None, "dp", "tensor"),
        P(None, None, "dp", "tensor"),
        P(),
        P(None, ("dp", "tensor"), None),
        P(None, ("dp", "tensor"), None),
        P(None, ("dp", "tensor"), None),
    )
    out_specs = (
        P(None, None, "dp", "tensor"),
        P(None, None, "dp", "tensor"),
        P(None, None, "dp", "tensor"),
        P(None, "dp", None),
        P(None, ("dp", "tensor"), None),
    )
    return jax.shard_map(
        per_device, mesh=mesh, in_specs=in_specs, out_specs=out_specs, check_vma=False
    )
```

```python
import math

import jax
import jax.numpy as jnp
from jax import lax
from jax.experimental import pallas as pl
from jax.experimental.pallas import tpu as pltpu
from jax.sharding import PartitionSpec as P


beta_one = 0.9
beta_two = 0.95
learn_rate = 0.02
decay_rate = 0.1
adam_eps = 1e-08
step_count = 10
norm_eps = 1e-06
lanes = 128
half = lanes // 2
megabyte = 1 << 20
kind_spans = (range(0, 3),)


def adam_update(master, moment_one, moment_two, gradients, clip_factor):
    scaled = gradients.astype(jnp.float32) * clip_factor
    first_moment = beta_one * moment_one + (1.0 - beta_one) * scaled
    second = beta_two * moment_two + (1.0 - beta_two) * scaled * scaled
    first_fix = 1.0 - beta_one**step_count
    second_fix = 1.0 - beta_two**step_count
    update = first_moment / first_fix / (jnp.sqrt(second / second_fix) + adam_eps)
    return (master - learn_rate * (update + decay_rate * master), first_moment, second)


def exchange(value, offset, member_count):
    return lax.ppermute(value, "dp", [(i, i ^ offset) for i in range(member_count)])


def stage_offsets(member_count):
    bits = member_count.bit_length() - 1
    assert 1 << bits == member_count
    pair = bits % 2
    return (pair, [[k << b for k in range(4)] for b in range(pair, bits, 2)])


hbm = pl.BlockSpec(memory_space=pltpu.HBM)
vmem = pl.BlockSpec(memory_space=pltpu.VMEM)


def call(kernel, out_shape, limit=24, **options):
    return pl.pallas_call(
        kernel,
        out_shape=out_shape,
        compiler_params=pltpu.CompilerParams(vmem_limit_bytes=limit * megabyte),
        **options,
    )


def prepare(gradients, hidden_in, norm_gain, expert_ids, route_weights, receivers):
    steps, row_count, model_width = hidden_in.shape
    top_count = expert_ids.shape[2]
    flat = gradients.reshape(-1, gradients.shape[-1])
    chunks = 6
    extent = flat.shape[0] // chunks

    def kernel(*refs):
        values, sources, sums, out, buffer = refs[0], refs[1:5], refs[5], refs[6], refs[7]
        buffers, done, arrived = refs[8:12], refs[12], refs[13]
        copies = [
            pltpu.make_async_copy(source, target, done.at[i])
            for i, (source, target) in enumerate(zip(sources, buffers))
        ]
        reads = [
            pltpu.make_async_copy(
                values.at[pl.ds(i * extent, extent)], buffer.at[i], arrived.at[i]
            )
            for i in range(chunks)
        ]
        for copy in copies + reads:
            copy.start()
        for copy in copies:
            copy.wait()
        hidden, gain, ids, gates = buffers
        rows = jnp.concatenate([hidden[s].astype(jnp.float32) for s in range(steps)], axis=0)
        factor = lax.rsqrt(jnp.mean(rows * rows, axis=1, keepdims=True) + norm_eps)
        out[:, :model_width] = (rows * factor * gain[...]).astype(jnp.bfloat16)
        lane = lax.rem(lax.broadcasted_iota(jnp.int32, (row_count, lanes), 1), half)
        diagonal = lax.broadcasted_iota(
            jnp.int32, (row_count, row_count), 0
        ) == lax.broadcasted_iota(jnp.int32, (row_count, row_count), 1)
        parts = []
        for s in range(steps):
            shares = gates[s] / jnp.sum(gates[s], axis=0, keepdims=True)
            mixed = jnp.zeros((row_count, lanes), jnp.float32)
            for k in range(top_count):
                named = jnp.where(diagonal, ids[s][k : k + 1], 0)
                share = jnp.where(diagonal, shares[k : k + 1], 0.0)
                mixed = mixed + jnp.where(
                    lane == jnp.sum(named, axis=1, keepdims=True),
                    jnp.sum(share, axis=1, keepdims=True),
                    0.0,
                )
            parts.append(mixed)
        combine = jnp.concatenate(parts, axis=0)
        lane = lax.broadcasted_iota(jnp.int32, combine.shape, 1)
        high = combine.astype(jnp.bfloat16).astype(jnp.float32)
        out[:, model_width:] = jnp.where(lane < half, high, combine - high).astype(jnp.bfloat16)
        total = jnp.zeros((8, flat.shape[1]), jnp.float32)
        for i, read in enumerate(reads):
            read.wait()
            widened = buffer[i].astype(jnp.float32)
            total = total + jnp.sum((widened * widened).reshape(-1, *total.shape), axis=0)
        sums[...] = jnp.full(sums.shape, jnp.sum(total), jnp.float32)

    arrays = (
        hidden_in,
        norm_gain.reshape(1, model_width),
        expert_ids.transpose(0, 2, 1),
        route_weights.transpose(0, 2, 1),
    )
    return call(
        kernel,
        (
            jax.ShapeDtypeStruct((receivers, 1, lanes), jnp.float32),
            jax.ShapeDtypeStruct((steps * row_count, model_width + lanes), jnp.bfloat16),
        ),
        limit=60,
        in_specs=[hbm] * 5,
        scratch_shapes=[pltpu.VMEM((chunks, extent, flat.shape[1]), flat.dtype)]
        + [pltpu.VMEM(array.shape, array.dtype) for array in arrays]
        + [pltpu.SemaphoreType.DMA((4,)), pltpu.SemaphoreType.DMA((chunks,))],
    )(flat, *arrays)


def expert_parts(row_blocks, weight_sets, hidden_total):
    expert_count, local_units, model_width = weight_sets[0][0].shape[1:]
    block_rows = row_blocks[0].shape[0]
    block_count, set_count, piece_count = len(row_blocks), len(weight_sets), len(weight_sets[0])
    pieces = [piece for weights in weight_sets for piece in weights]
    where = [(i, k) for i, piece in enumerate(weight_sets[0]) for k in range(piece.shape[0])]
    set_units = expert_count * local_units
    scale = 1.0 / math.sqrt(model_width)
    contract = (((1,), (1,)), ((), ()))

    def kernel(*refs):
        blocks, refs = refs[:block_count], refs[block_count:]
        held, outs = refs[: piece_count * set_count], refs[piece_count * set_count :]
        inputs = jnp.concatenate([b[...] for b in blocks], axis=0)
        rows, packed = inputs[:, :model_width], inputs[:, model_width:]

        def matrix(which):
            piece, kind = where[which]
            return jnp.concatenate(
                [
                    held[member * piece_count + piece][kind].reshape(set_units, model_width)
                    for member in range(set_count)
                ],
                axis=0,
            )

        units = set_count * set_units
        lane = lax.broadcasted_iota(jnp.int32, (lanes, units), 0)
        unit = lax.broadcasted_iota(jnp.int32, (lanes, units), 1)
        owner = lax.rem(unit, set_units) // local_units
        spread = (lax.rem(lane, half) == owner).astype(jnp.bfloat16)
        mix = jnp.dot(packed, spread, preferred_element_type=jnp.float32)
        gate = lax.dot_general(rows, matrix(0), contract, preferred_element_type=jnp.float32)
        up = lax.dot_general(rows, matrix(1), contract, preferred_element_type=jnp.float32)
        gate = gate * scale
        active = (gate / (1.0 + jnp.exp(-gate)) * (up * scale) * mix).astype(jnp.bfloat16)
        result = jnp.dot(active, matrix(2), preferred_element_type=jnp.float32)
        result = result * (1.0 / math.sqrt(hidden_total))
        for index, out in enumerate(outs):
            part = result[index * block_rows : (index + 1) * block_rows]
            out[...] = part.astype(out.dtype)

    shapes = [
        jax.ShapeDtypeStruct((block_rows, model_width), jnp.bfloat16 if b else jnp.float32)
        for b in range(block_count)
    ]
    return call(kernel, shapes, limit=40)(*row_blocks, *pieces)


def packing(strip_width):
    return max(1, 8 // strip_width)


def serve_step(master, moment_one, moment_two, gradients, sums, entries, strip_width, span):
    expert_count, local_units, local_width = master.shape[1:]
    first_kind, kinds = span.start, len(span)
    strips = local_units // strip_width
    pack = packing(strip_width)
    width = local_width // pack
    blocks = kinds * expert_count
    inputs = (master, moment_one, moment_two, gradients)
    first_scale = learn_rate / (1.0 - beta_one**step_count)
    second_scale = 1.0 / (1.0 - beta_two**step_count)

    def kernel(*refs):
        sources, shared, rounded, ordered = refs[:4], refs[4], refs[5], refs[6]
        buffers, packed, totals, got, put, summed = refs[7:11], *refs[11:16]
        fetch = pltpu.make_async_copy(shared, totals, summed.at[0])
        fetch.start()

        def place(b):
            return lax.div(b, expert_count), lax.rem(b, expert_count)

        def reads(b):
            k, e = place(b)
            return [
                pltpu.make_async_copy(source.at[first_kind + k, e], buffer.at[b], got.at[i, b])
                for i, (source, buffer) in enumerate(zip(sources, buffers))
            ]

        def write(b):
            k, e = place(b)
            return pltpu.make_async_copy(
                packed.at[b], ordered.at[pl.ds(e * strips, strips), k], put.at[b]
            )

        def issue(b, carry):
            for copy in reads(b):
                copy.start()
            return carry

        lax.fori_loop(0, blocks, issue, 0)
        fetch.wait()
        squares = jnp.sum(totals[:, :, :1])
        clip = jnp.minimum(1.0, lax.rsqrt(jnp.full((1, 1), squares) / entries + norm_eps))
        one_slope = clip * ((1.0 - beta_one) * first_scale)
        two_slope = clip * clip * ((1.0 - beta_two) * second_scale)

        def step(b, carry):
            for copy in reads(b):
                copy.wait()
            k, e = place(b)
            grad = buffers[3][b].astype(jnp.float32)
            top = buffers[1][b] * (beta_one * first_scale) + grad * one_slope
            square = buffers[2][b] * (beta_two * second_scale) + grad * grad * two_slope
            bottom = square * lax.rsqrt(square) + adam_eps
            new = buffers[0][b] * (1.0 - learn_rate * decay_rate) - top / bottom
            rounded[k, e] = new.astype(jnp.bfloat16)
            for t in range(strips):
                strip = new[t * strip_width : (t + 1) * strip_width]
                packed[b, t] = jnp.concatenate(
                    [strip[:, j * width : (j + 1) * width] for j in range(pack)], axis=0
                ).astype(jnp.bfloat16)
            write(b).start()
            return carry

        lax.fori_loop(0, blocks, step, 0)

        def finish(b, carry):
            write(b).wait()
            return carry

        lax.fori_loop(0, blocks, finish, 0)

    own = (local_units, local_width)
    return call(
        kernel,
        (
            jax.ShapeDtypeStruct((kinds,) + master.shape[1:], jnp.bfloat16),
            jax.ShapeDtypeStruct(
                (expert_count * strips, kinds, pack * strip_width, width), jnp.bfloat16
            ),
        ),
        limit=60,
        in_specs=[hbm] * 5,
        out_specs=(vmem, hbm),
        scratch_shapes=[pltpu.VMEM((blocks,) + own, array.dtype) for array in inputs]
        + [
            pltpu.VMEM((blocks, strips, pack * strip_width, width), jnp.bfloat16),
            pltpu.VMEM(sums.shape, sums.dtype),
            pltpu.SemaphoreType.DMA((4, blocks)),
            pltpu.SemaphoreType.DMA((blocks,)),
            pltpu.SemaphoreType.DMA((1,)),
        ],
    )(*inputs, sums)


def join_strips(owned, strip_width, first_kind, served):
    member_count, kinds, depth, width = owned.shape
    behind = [] if served is None else [served]
    pack = depth // strip_width
    split = 2
    members = member_count // split
    extent = members * strip_width

    def kernel(source, *refs):
        out, arrived, joined, got, put = refs[len(behind) :]

        def place(b):
            return lax.div(b, split), lax.rem(b, split)

        def read(b):
            k, h = place(b)
            return pltpu.make_async_copy(
                source.at[pl.ds(h * members, members), k], arrived.at[b], got.at[b]
            )

        def write(b):
            k, h = place(b)
            return pltpu.make_async_copy(
                joined.at[b], out.at[first_kind + k, pl.ds(h * extent, extent)], put.at[b]
            )

        for b in range(kinds * split):
            read(b).start()

        def step(b, carry):
            read(b).wait()
            for m in range(members // pack):
                group = [arrived[b, m * pack + g].astype(jnp.float32) for g in range(pack)]
                for j in range(pack):
                    joined[b, m * depth : (m + 1) * depth, j * width : (j + 1) * width] = (
                        jnp.concatenate(
                            [strip[j * strip_width : (j + 1) * strip_width] for strip in group],
                            axis=0,
                        ).astype(jnp.bfloat16)
                    )
            write(b).start()
            return carry

        lax.fori_loop(0, kinds * split, step, 0)
        for b in range(kinds * split):
            write(b).wait()

    return call(
        kernel,
        jax.ShapeDtypeStruct((3, member_count * strip_width, width * pack), jnp.bfloat16),
        input_output_aliases={1: 0} if behind else {},
        in_specs=[hbm] * (1 + len(behind)),
        out_specs=hbm,
        scratch_shapes=[
            pltpu.VMEM((kinds * split, members, depth, width), jnp.bfloat16),
            pltpu.VMEM((kinds * split, extent, width * pack), jnp.bfloat16),
            pltpu.SemaphoreType.DMA((kinds * split,)),
            pltpu.SemaphoreType.DMA((kinds * split,)),
        ],
    )(owned, *behind)


def per_device(
    master, moment_one, moment_two, gradients, norm_gain, hidden_in, expert_ids, route_weights
):
    slice_count = lax.axis_size("tensor")
    member_count = lax.axis_size("dp")
    expert_count = master.shape[1]
    local_units = master.shape[2]
    local_width = master.shape[3]
    hidden_total = local_units * member_count
    model_width = local_width * slice_count
    entries = 3 * expert_count * hidden_total * model_width
    pair, stages = stage_offsets(member_count)

    sums, gathered = prepare(
        gradients, hidden_in, norm_gain, expert_ids, route_weights, member_count
    )
    for place, offsets in enumerate(reversed(stages)):
        blocks = [gathered] + [exchange(gathered, k, member_count) for k in offsets[1:]]
        if place < len(stages) - 1:
            gathered = jnp.concatenate(blocks, axis=0)

    sums = lax.all_to_all(sums, "dp", split_axis=0, concat_axis=0, tiled=True)
    if slice_count > 1:
        sums = lax.psum(sums, "tensor")
    group_size = member_count // expert_count
    strip_width = local_units // group_size
    pack = packing(strip_width)
    weight_sets = [[] for _ in range(1 + pair)]
    arrived = []
    for span in kind_spans:
        whole, ordered = serve_step(
            master, moment_one, moment_two, gradients, sums, entries, strip_width, span
        )
        if slice_count > 1:
            whole = lax.all_gather(whole, "tensor", axis=3, tiled=True)
            ordered = whole.reshape(
                len(span), member_count, strip_width, pack, model_width // pack
            )
            ordered = ordered.transpose(1, 0, 3, 2, 4).reshape(
                member_count, len(span), pack * strip_width, model_width // pack
            )
        weight_sets[0].append(whole)
        if pair:
            weight_sets[1].append(exchange(whole, pair, member_count))
        arrived.append(
            lax.all_to_all(ordered, "dp", split_axis=0, concat_axis=0, tiled=True)
        )
    served = None
    for span, owned in zip(kind_spans, arrived):
        served = join_strips(owned, strip_width, span.start, served)

    squares = jnp.sum(sums[:, 0, 0])
    clip_factor = jnp.minimum(1.0, lax.rsqrt(squares / entries + norm_eps))
    new_master, new_one, new_two = adam_update(
        master, moment_one, moment_two, gradients, clip_factor
    )
    parts = expert_parts(blocks, weight_sets, hidden_total)
    for place, offsets in enumerate(stages):
        summed = parts[0]
        for index, k in enumerate(offsets[1:], 1):
            summed = summed + exchange(parts[index], k, member_count).astype(jnp.float32)
        if place < len(stages) - 1:
            extent = summed.shape[0] // len(offsets)
            pieces = [summed[i * extent : (i + 1) * extent] for i in range(len(offsets))]
            parts = pieces[:1] + [piece.astype(jnp.bfloat16) for piece in pieces[1:]]
    decoded = hidden_in.astype(jnp.float32) + summed.reshape(hidden_in.shape)
    return (new_master, new_one, new_two, served, decoded.astype(jnp.bfloat16))


def solution(mesh):
    in_specs = (
        P(None, None, "dp", "tensor"),
        P(None, None, "dp", "tensor"),
        P(None, None, "dp", "tensor"),
        P(None, None, "dp", "tensor"),
        P(),
        P(None, ("dp", "tensor"), None),
        P(None, ("dp", "tensor"), None),
        P(None, ("dp", "tensor"), None),
    )
    out_specs = (
        P(None, None, "dp", "tensor"),
        P(None, None, "dp", "tensor"),
        P(None, None, "dp", "tensor"),
        P(None, "dp", None),
        P(None, ("dp", "tensor"), None),
    )

    return jax.shard_map(
        per_device, mesh=mesh, in_specs=in_specs, out_specs=out_specs, check_vma=False
    )
```

```python
import math

import jax
import jax.numpy as jnp
from jax import lax
from jax.experimental import pallas as pl
from jax.experimental.pallas import tpu as pltpu
from jax.sharding import PartitionSpec as P


beta_one = 0.9
beta_two = 0.95
learn_rate = 0.02
decay_rate = 0.1
adam_eps = 1e-08
step_count = 10
norm_eps = 1e-06
lanes = 128
half = lanes // 2
megabyte = 1 << 20
kind_spans = (range(0, 3),)


def adam_update(master, moment_one, moment_two, gradients, clip_factor):
    scaled = gradients.astype(jnp.float32) * clip_factor
    first_moment = beta_one * moment_one + (1.0 - beta_one) * scaled
    second = beta_two * moment_two + (1.0 - beta_two) * scaled * scaled
    first_fix = 1.0 - beta_one**step_count
    second_fix = 1.0 - beta_two**step_count
    update = first_moment / first_fix / (jnp.sqrt(second / second_fix) + adam_eps)
    return (master - learn_rate * (update + decay_rate * master), first_moment, second)


def exchange(value, offset, member_count):
    return lax.ppermute(value, "dp", [(i, i ^ offset) for i in range(member_count)])


def stage_offsets(member_count):
    bits = member_count.bit_length() - 1
    assert 1 << bits == member_count
    pair = bits % 2
    return (pair, [[k << b for k in range(4)] for b in range(pair, bits, 2)])


hbm = pl.BlockSpec(memory_space=pltpu.HBM)
vmem = pl.BlockSpec(memory_space=pltpu.VMEM)


def call(kernel, out_shape, limit=24, **options):
    return pl.pallas_call(
        kernel,
        out_shape=out_shape,
        compiler_params=pltpu.CompilerParams(vmem_limit_bytes=limit * megabyte),
        **options,
    )


def prepare(gradients, hidden_in, norm_gain, expert_ids, route_weights, receivers):
    steps, row_count, model_width = hidden_in.shape
    top_count = expert_ids.shape[2]
    flat = gradients.reshape(-1, gradients.shape[-1])
    chunks = 6
    extent = flat.shape[0] // chunks

    def kernel(*refs):
        values, sources, sums, out, buffer = refs[0], refs[1:5], refs[5], refs[6], refs[7]
        buffers, done, arrived = refs[8:12], refs[12], refs[13]
        copies = [
            pltpu.make_async_copy(source, target, done.at[i])
            for i, (source, target) in enumerate(zip(sources, buffers))
        ]
        reads = [
            pltpu.make_async_copy(
                values.at[pl.ds(i * extent, extent)], buffer.at[i], arrived.at[i]
            )
            for i in range(chunks)
        ]
        for copy in copies + reads:
            copy.start()
        for copy in copies:
            copy.wait()
        hidden, gain, ids, gates = buffers
        rows = jnp.concatenate([hidden[s].astype(jnp.float32) for s in range(steps)], axis=0)
        factor = lax.rsqrt(jnp.mean(rows * rows, axis=1, keepdims=True) + norm_eps)
        out[:, :model_width] = (rows * factor * gain[...]).astype(jnp.bfloat16)
        lane = lax.rem(lax.broadcasted_iota(jnp.int32, (row_count, lanes), 1), half)
        diagonal = lax.broadcasted_iota(
            jnp.int32, (row_count, row_count), 0
        ) == lax.broadcasted_iota(jnp.int32, (row_count, row_count), 1)
        parts = []
        for s in range(steps):
            shares = gates[s] / jnp.sum(gates[s], axis=0, keepdims=True)
            mixed = jnp.zeros((row_count, lanes), jnp.float32)
            for k in range(top_count):
                named = jnp.where(diagonal, ids[s][k : k + 1], 0)
                share = jnp.where(diagonal, shares[k : k + 1], 0.0)
                mixed = mixed + jnp.where(
                    lane == jnp.sum(named, axis=1, keepdims=True),
                    jnp.sum(share, axis=1, keepdims=True),
                    0.0,
                )
            parts.append(mixed)
        combine = jnp.concatenate(parts, axis=0)
        lane = lax.broadcasted_iota(jnp.int32, combine.shape, 1)
        high = combine.astype(jnp.bfloat16).astype(jnp.float32)
        out[:, model_width:] = jnp.where(lane < half, high, combine - high).astype(jnp.bfloat16)
        total = jnp.zeros((8, flat.shape[1]), jnp.float32)
        for i, read in enumerate(reads):
            read.wait()
            widened = buffer[i].astype(jnp.float32)
            total = total + jnp.sum((widened * widened).reshape(-1, *total.shape), axis=0)
        sums[...] = jnp.full(sums.shape, jnp.sum(total), jnp.float32)

    arrays = (
        hidden_in,
        norm_gain.reshape(1, model_width),
        expert_ids.transpose(0, 2, 1),
        route_weights.transpose(0, 2, 1),
    )
    return call(
        kernel,
        (
            jax.ShapeDtypeStruct((receivers, 1, lanes), jnp.float32),
            jax.ShapeDtypeStruct((steps * row_count, model_width + lanes), jnp.bfloat16),
        ),
        limit=60,
        in_specs=[hbm] * 5,
        scratch_shapes=[pltpu.VMEM((chunks, extent, flat.shape[1]), flat.dtype)]
        + [pltpu.VMEM(array.shape, array.dtype) for array in arrays]
        + [pltpu.SemaphoreType.DMA((4,)), pltpu.SemaphoreType.DMA((chunks,))],
    )(flat, *arrays)


def expert_parts(row_blocks, weight_sets, hidden_total):
    expert_count, local_units, model_width = weight_sets[0][0].shape[1:]
    block_rows = row_blocks[0].shape[0]
    block_count, set_count, piece_count = len(row_blocks), len(weight_sets), len(weight_sets[0])
    pieces = [piece for weights in weight_sets for piece in weights]
    where = [(i, k) for i, piece in enumerate(weight_sets[0]) for k in range(piece.shape[0])]
    set_units = expert_count * local_units
    scale = 1.0 / math.sqrt(model_width)
    contract = (((1,), (1,)), ((), ()))

    def kernel(*refs):
        blocks, refs = refs[:block_count], refs[block_count:]
        held, outs = refs[: piece_count * set_count], refs[piece_count * set_count :]
        inputs = jnp.concatenate([b[...] for b in blocks], axis=0)
        rows, packed = inputs[:, :model_width], inputs[:, model_width:]

        def matrix(which):
            piece, kind = where[which]
            return jnp.concatenate(
                [
                    held[member * piece_count + piece][kind].reshape(set_units, model_width)
                    for member in range(set_count)
                ],
                axis=0,
            )

        units = set_count * set_units
        lane = lax.broadcasted_iota(jnp.int32, (lanes, units), 0)
        unit = lax.broadcasted_iota(jnp.int32, (lanes, units), 1)
        owner = lax.rem(unit, set_units) // local_units
        spread = (lax.rem(lane, half) == owner).astype(jnp.bfloat16)
        mix = jnp.dot(packed, spread, preferred_element_type=jnp.float32)
        gate = lax.dot_general(rows, matrix(0), contract, preferred_element_type=jnp.float32)
        up = lax.dot_general(rows, matrix(1), contract, preferred_element_type=jnp.float32)
        gate = gate * scale
        active = (gate / (1.0 + jnp.exp(-gate)) * (up * scale) * mix).astype(jnp.bfloat16)
        result = jnp.dot(active, matrix(2), preferred_element_type=jnp.float32)
        result = result * (1.0 / math.sqrt(hidden_total))
        for index, out in enumerate(outs):
            part = result[index * block_rows : (index + 1) * block_rows]
            out[...] = part.astype(out.dtype)

    shapes = [
        jax.ShapeDtypeStruct((block_rows, model_width), jnp.bfloat16 if b else jnp.float32)
        for b in range(block_count)
    ]
    return call(kernel, shapes, limit=40)(*row_blocks, *pieces)


def packing(strip_width):
    return max(1, 8 // strip_width)


def serve_step(master, moment_one, moment_two, gradients, sums, entries, strip_width, span):
    expert_count, local_units, local_width = master.shape[1:]
    first_kind, kinds = span.start, len(span)
    strips = local_units // strip_width
    pack = packing(strip_width)
    width = local_width // pack
    blocks = kinds * expert_count
    inputs = (master, moment_one, moment_two, gradients)
    first_scale = learn_rate / (1.0 - beta_one**step_count)
    second_scale = 1.0 / (1.0 - beta_two**step_count)

    def kernel(*refs):
        sources, shared, rounded, ordered = refs[:4], refs[4], refs[5], refs[6]
        buffers, packed, plain, totals, got, put, summed = refs[7:11], *refs[11:17]
        fetch = pltpu.make_async_copy(shared, totals, summed.at[0])
        fetch.start()

        def place(b):
            return lax.div(b, expert_count), lax.rem(b, expert_count)

        def reads(b):
            k, e = place(b)
            return [
                pltpu.make_async_copy(source.at[first_kind + k, e], buffer.at[b], got.at[i, b])
                for i, (source, buffer) in enumerate(zip(sources, buffers))
            ]

        def writes(b):
            k, e = place(b)
            return [
                pltpu.make_async_copy(
                    packed.at[b], ordered.at[pl.ds(e * strips, strips), k], put.at[0, b]
                ),
                pltpu.make_async_copy(plain.at[b], rounded.at[k, e], put.at[1, b]),
            ]

        def issue(b, carry):
            for copy in reads(b):
                copy.start()
            return carry

        lax.fori_loop(0, blocks, issue, 0)
        fetch.wait()
        squares = jnp.sum(totals[:, :, :1])
        clip = jnp.minimum(1.0, lax.rsqrt(jnp.full((1, 1), squares) / entries + norm_eps))
        one_slope = clip * ((1.0 - beta_one) * first_scale)
        two_slope = clip * clip * ((1.0 - beta_two) * second_scale)

        def step(b, carry):
            for copy in reads(b):
                copy.wait()
            k, e = place(b)
            grad = buffers[3][b].astype(jnp.float32)
            top = buffers[1][b] * (beta_one * first_scale) + grad * one_slope
            square = buffers[2][b] * (beta_two * second_scale) + grad * grad * two_slope
            bottom = square * lax.rsqrt(square) + adam_eps
            new = buffers[0][b] * (1.0 - learn_rate * decay_rate) - top / bottom
            plain[b] = new.astype(jnp.bfloat16)
            for t in range(strips):
                strip = new[t * strip_width : (t + 1) * strip_width]
                packed[b, t] = jnp.concatenate(
                    [strip[:, j * width : (j + 1) * width] for j in range(pack)], axis=0
                ).astype(jnp.bfloat16)
            for copy in writes(b):
                copy.start()
            return carry

        lax.fori_loop(0, blocks, step, 0)

        def finish(b, carry):
            for copy in writes(b):
                copy.wait()
            return carry

        lax.fori_loop(0, blocks, finish, 0)

    own = (local_units, local_width)
    return call(
        kernel,
        (
            jax.ShapeDtypeStruct((kinds,) + master.shape[1:], jnp.bfloat16),
            jax.ShapeDtypeStruct(
                (expert_count * strips, kinds, pack * strip_width, width), jnp.bfloat16
            ),
        ),
        limit=60,
        in_specs=[hbm] * 5,
        out_specs=(hbm, hbm),
        scratch_shapes=[pltpu.VMEM((blocks,) + own, array.dtype) for array in inputs]
        + [
            pltpu.VMEM((blocks, strips, pack * strip_width, width), jnp.bfloat16),
            pltpu.VMEM((blocks,) + own, jnp.bfloat16),
            pltpu.VMEM(sums.shape, sums.dtype),
            pltpu.SemaphoreType.DMA((4, blocks)),
            pltpu.SemaphoreType.DMA((2, blocks)),
            pltpu.SemaphoreType.DMA((1,)),
        ],
    )(*inputs, sums)


def join_strips(owned, strip_width, first_kind, served):
    member_count, kinds, depth, width = owned.shape
    behind = [] if served is None else [served]
    pack = depth // strip_width
    split = 2
    members = member_count // split
    extent = members * strip_width

    def kernel(source, *refs):
        out, arrived, joined, got, put = refs[len(behind) :]

        def place(b):
            return lax.div(b, split), lax.rem(b, split)

        def read(b):
            k, h = place(b)
            return pltpu.make_async_copy(
                source.at[pl.ds(h * members, members), k], arrived.at[b], got.at[b]
            )

        def write(b):
            k, h = place(b)
            return pltpu.make_async_copy(
                joined.at[b], out.at[first_kind + k, pl.ds(h * extent, extent)], put.at[b]
            )

        for b in range(kinds * split):
            read(b).start()

        def step(b, carry):
            read(b).wait()
            for m in range(members // pack):
                group = [arrived[b, m * pack + g].astype(jnp.float32) for g in range(pack)]
                for j in range(pack):
                    joined[b, m * depth : (m + 1) * depth, j * width : (j + 1) * width] = (
                        jnp.concatenate(
                            [strip[j * strip_width : (j + 1) * strip_width] for strip in group],
                            axis=0,
                        ).astype(jnp.bfloat16)
                    )
            write(b).start()
            return carry

        lax.fori_loop(0, kinds * split, step, 0)
        for b in range(kinds * split):
            write(b).wait()

    return call(
        kernel,
        jax.ShapeDtypeStruct((3, member_count * strip_width, width * pack), jnp.bfloat16),
        input_output_aliases={1: 0} if behind else {},
        in_specs=[hbm] * (1 + len(behind)),
        out_specs=hbm,
        scratch_shapes=[
            pltpu.VMEM((kinds * split, members, depth, width), jnp.bfloat16),
            pltpu.VMEM((kinds * split, extent, width * pack), jnp.bfloat16),
            pltpu.SemaphoreType.DMA((kinds * split,)),
            pltpu.SemaphoreType.DMA((kinds * split,)),
        ],
    )(owned, *behind)


def per_device(
    master, moment_one, moment_two, gradients, norm_gain, hidden_in, expert_ids, route_weights
):
    slice_count = lax.axis_size("tensor")
    member_count = lax.axis_size("dp")
    expert_count = master.shape[1]
    local_units = master.shape[2]
    local_width = master.shape[3]
    hidden_total = local_units * member_count
    model_width = local_width * slice_count
    entries = 3 * expert_count * hidden_total * model_width
    pair, stages = stage_offsets(member_count)

    sums, gathered = prepare(
        gradients, hidden_in, norm_gain, expert_ids, route_weights, member_count
    )
    for place, offsets in enumerate(reversed(stages)):
        others = [exchange(gathered, k, member_count) for k in reversed(offsets[1:])]
        blocks = [gathered] + others[::-1]
        if place < len(stages) - 1:
            gathered = jnp.concatenate(blocks, axis=0)

    sums = lax.all_to_all(sums, "dp", split_axis=0, concat_axis=0, tiled=True)
    if slice_count > 1:
        sums = lax.psum(sums, "tensor")
    group_size = member_count // expert_count
    strip_width = local_units // group_size
    pack = packing(strip_width)
    weight_sets = [[] for _ in range(1 + pair)]
    arrived = []
    for span in kind_spans:
        whole, ordered = serve_step(
            master, moment_one, moment_two, gradients, sums, entries, strip_width, span
        )
        if slice_count > 1:
            whole = lax.all_gather(whole, "tensor", axis=3, tiled=True)
            ordered = whole.reshape(
                len(span), member_count, strip_width, pack, model_width // pack
            )
            ordered = ordered.transpose(1, 0, 3, 2, 4).reshape(
                member_count, len(span), pack * strip_width, model_width // pack
            )
        weight_sets[0].append(whole)
        if pair:
            weight_sets[1].append(exchange(whole, pair, member_count))
        arrived.append(
            lax.all_to_all(ordered, "dp", split_axis=0, concat_axis=0, tiled=True)
        )
    served = None
    for span, owned in zip(kind_spans, arrived):
        served = join_strips(owned, strip_width, span.start, served)

    squares = jnp.sum(sums[:, 0, 0])
    clip_factor = jnp.minimum(1.0, lax.rsqrt(squares / entries + norm_eps))
    new_master, new_one, new_two = adam_update(
        master, moment_one, moment_two, gradients, clip_factor
    )
    parts = expert_parts(blocks, weight_sets, hidden_total)
    for place, offsets in enumerate(stages):
        summed = parts[0]
        for index, k in reversed(list(enumerate(offsets[1:], 1))):
            summed = summed + exchange(parts[index], k, member_count).astype(jnp.float32)
        if place < len(stages) - 1:
            extent = summed.shape[0] // len(offsets)
            pieces = [summed[i * extent : (i + 1) * extent] for i in range(len(offsets))]
            parts = pieces[:1] + [piece.astype(jnp.bfloat16) for piece in pieces[1:]]
    decoded = hidden_in.astype(jnp.float32) + summed.reshape(hidden_in.shape)
    return (new_master, new_one, new_two, served, decoded.astype(jnp.bfloat16))


def solution(mesh):
    in_specs = (
        P(None, None, "dp", "tensor"),
        P(None, None, "dp", "tensor"),
        P(None, None, "dp", "tensor"),
        P(None, None, "dp", "tensor"),
        P(),
        P(None, ("dp", "tensor"), None),
        P(None, ("dp", "tensor"), None),
        P(None, ("dp", "tensor"), None),
    )
    out_specs = (
        P(None, None, "dp", "tensor"),
        P(None, None, "dp", "tensor"),
        P(None, None, "dp", "tensor"),
        P(None, "dp", None),
        P(None, ("dp", "tensor"), None),
    )

    return jax.shard_map(
        per_device, mesh=mesh, in_specs=in_specs, out_specs=out_specs, check_vma=False
    )
```

```python
import math

import jax
import jax.numpy as jnp
from jax import lax
from jax.experimental import pallas as pl
from jax.experimental.pallas import tpu as pltpu
from jax.sharding import PartitionSpec as P


beta_one = 0.9
beta_two = 0.95
learn_rate = 0.02
decay_rate = 0.1
adam_eps = 1e-08
step_count = 10
norm_eps = 1e-06
lanes = 128
half = lanes // 2
megabyte = 1 << 20
kind_spans = (range(0, 3),)


def adam_update(master, moment_one, moment_two, gradients, clip_factor):
    scaled = gradients.astype(jnp.float32) * clip_factor
    first_moment = beta_one * moment_one + (1.0 - beta_one) * scaled
    second = beta_two * moment_two + (1.0 - beta_two) * scaled * scaled
    first_fix = 1.0 - beta_one**step_count
    second_fix = 1.0 - beta_two**step_count
    update = first_moment / first_fix / (jnp.sqrt(second / second_fix) + adam_eps)
    return (master - learn_rate * (update + decay_rate * master), first_moment, second)


def exchange(value, offset, member_count):
    return lax.ppermute(value, "dp", [(i, i ^ offset) for i in range(member_count)])


def stage_offsets(member_count):
    bits = member_count.bit_length() - 1
    assert 1 << bits == member_count
    pair = bits % 2
    return (pair, [[k << b for k in range(4)] for b in range(pair, bits, 2)])


hbm = pl.BlockSpec(memory_space=pltpu.HBM)
vmem = pl.BlockSpec(memory_space=pltpu.VMEM)


def call(kernel, out_shape, limit=24, **options):
    return pl.pallas_call(
        kernel,
        out_shape=out_shape,
        compiler_params=pltpu.CompilerParams(vmem_limit_bytes=limit * megabyte),
        **options,
    )


def prepare(gradients, hidden_in, norm_gain, expert_ids, route_weights, receivers):
    steps, row_count, model_width = hidden_in.shape
    top_count = expert_ids.shape[2]
    flat = gradients.reshape(-1, gradients.shape[-1])
    chunks = 6
    extent = flat.shape[0] // chunks

    def kernel(*refs):
        values, sources, sums, out, buffer = refs[0], refs[1:5], refs[5], refs[6], refs[7]
        buffers, done, arrived = refs[8:12], refs[12], refs[13]
        copies = [
            pltpu.make_async_copy(source, target, done.at[i])
            for i, (source, target) in enumerate(zip(sources, buffers))
        ]
        reads = [
            pltpu.make_async_copy(
                values.at[pl.ds(i * extent, extent)], buffer.at[i], arrived.at[i]
            )
            for i in range(chunks)
        ]
        for copy in copies + reads:
            copy.start()
        for copy in copies:
            copy.wait()
        hidden, gain, ids, gates = buffers
        rows = jnp.concatenate([hidden[s].astype(jnp.float32) for s in range(steps)], axis=0)
        factor = lax.rsqrt(jnp.mean(rows * rows, axis=1, keepdims=True) + norm_eps)
        out[:, :model_width] = (rows * factor * gain[...]).astype(jnp.bfloat16)
        lane = lax.rem(lax.broadcasted_iota(jnp.int32, (row_count, lanes), 1), half)
        diagonal = lax.broadcasted_iota(
            jnp.int32, (row_count, row_count), 0
        ) == lax.broadcasted_iota(jnp.int32, (row_count, row_count), 1)
        parts = []
        for s in range(steps):
            shares = gates[s] / jnp.sum(gates[s], axis=0, keepdims=True)
            mixed = jnp.zeros((row_count, lanes), jnp.float32)
            for k in range(top_count):
                named = jnp.where(diagonal, ids[s][k : k + 1], 0)
                share = jnp.where(diagonal, shares[k : k + 1], 0.0)
                mixed = mixed + jnp.where(
                    lane == jnp.sum(named, axis=1, keepdims=True),
                    jnp.sum(share, axis=1, keepdims=True),
                    0.0,
                )
            parts.append(mixed)
        combine = jnp.concatenate(parts, axis=0)
        lane = lax.broadcasted_iota(jnp.int32, combine.shape, 1)
        high = combine.astype(jnp.bfloat16).astype(jnp.float32)
        out[:, model_width:] = jnp.where(lane < half, high, combine - high).astype(jnp.bfloat16)
        total = jnp.zeros((8, flat.shape[1]), jnp.float32)
        for i, read in enumerate(reads):
            read.wait()
            widened = buffer[i].astype(jnp.float32)
            total = total + jnp.sum((widened * widened).reshape(-1, *total.shape), axis=0)
        sums[...] = jnp.full(sums.shape, jnp.sum(total), jnp.float32)

    arrays = (
        hidden_in,
        norm_gain.reshape(1, model_width),
        expert_ids.transpose(0, 2, 1),
        route_weights.transpose(0, 2, 1),
    )
    return call(
        kernel,
        (
            jax.ShapeDtypeStruct((receivers, 1, lanes), jnp.float32),
            jax.ShapeDtypeStruct((steps * row_count, model_width + lanes), jnp.bfloat16),
        ),
        limit=54,
        in_specs=[hbm] * 5,
        scratch_shapes=[pltpu.VMEM((chunks, extent, flat.shape[1]), flat.dtype)]
        + [pltpu.VMEM(array.shape, array.dtype) for array in arrays]
        + [pltpu.SemaphoreType.DMA((4,)), pltpu.SemaphoreType.DMA((chunks,))],
    )(flat, *arrays)


def expert_parts(row_blocks, weight_sets, hidden_total):
    expert_count, local_units, model_width = weight_sets[0][0].shape[1:]
    block_rows = row_blocks[0].shape[0]
    block_count, set_count, piece_count = len(row_blocks), len(weight_sets), len(weight_sets[0])
    pieces = [piece for weights in weight_sets for piece in weights]
    where = [(i, k) for i, piece in enumerate(weight_sets[0]) for k in range(piece.shape[0])]
    set_units = expert_count * local_units
    scale = 1.0 / math.sqrt(model_width)
    contract = (((1,), (1,)), ((), ()))

    def kernel(*refs):
        blocks, refs = refs[:block_count], refs[block_count:]
        held, outs = refs[: piece_count * set_count], refs[piece_count * set_count :]
        inputs = jnp.concatenate([b[...] for b in blocks], axis=0)
        rows, packed = inputs[:, :model_width], inputs[:, model_width:]

        def matrix(which):
            piece, kind = where[which]
            return jnp.concatenate(
                [
                    held[member * piece_count + piece][kind].reshape(set_units, model_width)
                    for member in range(set_count)
                ],
                axis=0,
            )

        units = set_count * set_units
        lane = lax.broadcasted_iota(jnp.int32, (lanes, units), 0)
        unit = lax.broadcasted_iota(jnp.int32, (lanes, units), 1)
        owner = lax.rem(unit, set_units) // local_units
        spread = (lax.rem(lane, half) == owner).astype(jnp.bfloat16)
        mix = jnp.dot(packed, spread, preferred_element_type=jnp.float32)
        gate = lax.dot_general(rows, matrix(0), contract, preferred_element_type=jnp.float32)
        up = lax.dot_general(rows, matrix(1), contract, preferred_element_type=jnp.float32)
        gate = gate * scale
        active = (gate / (1.0 + jnp.exp(-gate)) * (up * scale) * mix).astype(jnp.bfloat16)
        result = jnp.dot(active, matrix(2), preferred_element_type=jnp.float32)
        result = result * (1.0 / math.sqrt(hidden_total))
        for index, out in enumerate(outs):
            part = result[index * block_rows : (index + 1) * block_rows]
            out[...] = part.astype(out.dtype)

    shapes = [
        jax.ShapeDtypeStruct((block_rows, model_width), jnp.bfloat16 if b else jnp.float32)
        for b in range(block_count)
    ]
    return call(kernel, shapes, limit=40)(*row_blocks, *pieces)


def packing(strip_width):
    return max(1, 8 // strip_width)


def serve_step(master, moment_one, moment_two, gradients, sums, entries, strip_width, span):
    expert_count, local_units, local_width = master.shape[1:]
    first_kind, kinds = span.start, len(span)
    strips = local_units // strip_width
    pack = packing(strip_width)
    width = local_width // pack
    blocks = kinds * expert_count
    inputs = (master, moment_one, moment_two, gradients)
    first_scale = learn_rate / (1.0 - beta_one**step_count)
    second_scale = 1.0 / (1.0 - beta_two**step_count)

    def kernel(*refs):
        sources, totals, rounded, ordered = refs[:4], refs[4], refs[5], refs[6]
        buffers, packed, plain, got, put = refs[7:11], *refs[11:15]

        def place(b):
            return lax.div(b, expert_count), lax.rem(b, expert_count)

        def reads(b):
            k, e = place(b)
            return [
                pltpu.make_async_copy(source.at[first_kind + k, e], buffer.at[b], got.at[i, b])
                for i, (source, buffer) in enumerate(zip(sources, buffers))
            ]

        def writes(b):
            k, e = place(b)
            return [
                pltpu.make_async_copy(
                    packed.at[b], ordered.at[pl.ds(e * strips, strips), k], put.at[0, b]
                ),
                pltpu.make_async_copy(plain.at[b], rounded.at[k, e], put.at[1, b]),
            ]

        def issue(b, carry):
            for copy in reads(b):
                copy.start()
            return carry

        lax.fori_loop(0, blocks, issue, 0)
        squares = jnp.sum(totals[:, :, :1])
        clip = jnp.minimum(1.0, lax.rsqrt(jnp.full((1, 1), squares) / entries + norm_eps))
        one_slope = clip * ((1.0 - beta_one) * first_scale)
        two_slope = clip * clip * ((1.0 - beta_two) * second_scale)

        def step(b, carry):
            for copy in reads(b):
                copy.wait()
            k, e = place(b)
            grad = buffers[3][b].astype(jnp.float32)
            top = buffers[1][b] * (beta_one * first_scale) + grad * one_slope
            square = buffers[2][b] * (beta_two * second_scale) + grad * grad * two_slope
            bottom = square * lax.rsqrt(square) + adam_eps
            new = buffers[0][b] * (1.0 - learn_rate * decay_rate) - top / bottom
            plain[b] = new.astype(jnp.bfloat16)
            for t in range(strips):
                strip = new[t * strip_width : (t + 1) * strip_width]
                packed[b, t] = jnp.concatenate(
                    [strip[:, j * width : (j + 1) * width] for j in range(pack)], axis=0
                ).astype(jnp.bfloat16)
            for copy in writes(b):
                copy.start()
            return carry

        lax.fori_loop(0, blocks, step, 0)

        def finish(b, carry):
            for copy in writes(b):
                copy.wait()
            return carry

        lax.fori_loop(0, blocks, finish, 0)

    own = (local_units, local_width)
    return call(
        kernel,
        (
            jax.ShapeDtypeStruct((kinds,) + master.shape[1:], jnp.bfloat16),
            jax.ShapeDtypeStruct(
                (expert_count * strips, kinds, pack * strip_width, width), jnp.bfloat16
            ),
        ),
        limit=53,
        in_specs=[hbm] * 4 + [vmem],
        out_specs=(hbm, hbm),
        scratch_shapes=[pltpu.VMEM((blocks,) + own, array.dtype) for array in inputs]
        + [
            pltpu.VMEM((blocks, strips, pack * strip_width, width), jnp.bfloat16),
            pltpu.VMEM((blocks,) + own, jnp.bfloat16),
            pltpu.SemaphoreType.DMA((4, blocks)),
            pltpu.SemaphoreType.DMA((2, blocks)),
        ],
    )(*inputs, sums)


def join_strips(owned, strip_width, first_kind, served):
    member_count, kinds, depth, width = owned.shape
    behind = [] if served is None else [served]
    pack = depth // strip_width
    split = 2
    members = member_count // split
    extent = members * strip_width

    def kernel(source, *refs):
        out, arrived, joined, got, put = refs[len(behind) :]

        def place(b):
            return lax.div(b, split), lax.rem(b, split)

        def read(b):
            k, h = place(b)
            return pltpu.make_async_copy(
                source.at[pl.ds(h * members, members), k], arrived.at[b], got.at[b]
            )

        def write(b):
            k, h = place(b)
            return pltpu.make_async_copy(
                joined.at[b], out.at[first_kind + k, pl.ds(h * extent, extent)], put.at[b]
            )

        for b in range(kinds * split):
            read(b).start()

        def step(b, carry):
            read(b).wait()
            for m in range(members // pack):
                group = [arrived[b, m * pack + g].astype(jnp.float32) for g in range(pack)]
                for j in range(pack):
                    joined[b, m * depth : (m + 1) * depth, j * width : (j + 1) * width] = (
                        jnp.concatenate(
                            [strip[j * strip_width : (j + 1) * strip_width] for strip in group],
                            axis=0,
                        ).astype(jnp.bfloat16)
                    )
            write(b).start()
            return carry

        lax.fori_loop(0, kinds * split, step, 0)
        for b in range(kinds * split):
            write(b).wait()

    return call(
        kernel,
        jax.ShapeDtypeStruct((3, member_count * strip_width, width * pack), jnp.bfloat16),
        input_output_aliases={1: 0} if behind else {},
        in_specs=[hbm] * (1 + len(behind)),
        out_specs=hbm,
        scratch_shapes=[
            pltpu.VMEM((kinds * split, members, depth, width), jnp.bfloat16),
            pltpu.VMEM((kinds * split, extent, width * pack), jnp.bfloat16),
            pltpu.SemaphoreType.DMA((kinds * split,)),
            pltpu.SemaphoreType.DMA((kinds * split,)),
        ],
    )(owned, *behind)


def per_device(
    master, moment_one, moment_two, gradients, norm_gain, hidden_in, expert_ids, route_weights
):
    slice_count = lax.axis_size("tensor")
    member_count = lax.axis_size("dp")
    expert_count = master.shape[1]
    local_units = master.shape[2]
    local_width = master.shape[3]
    hidden_total = local_units * member_count
    model_width = local_width * slice_count
    entries = 3 * expert_count * hidden_total * model_width
    pair, stages = stage_offsets(member_count)

    sums, gathered = prepare(
        gradients, hidden_in, norm_gain, expert_ids, route_weights, member_count
    )
    for place, offsets in enumerate(reversed(stages)):
        others = [exchange(gathered, k, member_count) for k in reversed(offsets[1:])]
        blocks = [gathered] + others[::-1]
        if place < len(stages) - 1:
            gathered = jnp.concatenate(blocks, axis=0)

    sums = lax.all_to_all(sums, "dp", split_axis=0, concat_axis=0, tiled=True)
    if slice_count > 1:
        sums = lax.psum(sums, "tensor")
    group_size = member_count // expert_count
    strip_width = local_units // group_size
    pack = packing(strip_width)
    weight_sets = [[] for _ in range(1 + pair)]
    arrived = []
    for span in kind_spans:
        whole, ordered = serve_step(
            master, moment_one, moment_two, gradients, sums, entries, strip_width, span
        )
        if slice_count > 1:
            whole = lax.all_gather(whole, "tensor", axis=3, tiled=True)
            ordered = whole.reshape(
                len(span), member_count, strip_width, pack, model_width // pack
            )
            ordered = ordered.transpose(1, 0, 3, 2, 4).reshape(
                member_count, len(span), pack * strip_width, model_width // pack
            )
        weight_sets[0].append(whole)
        if pair:
            weight_sets[1].append(exchange(whole, pair, member_count))
        arrived.append(
            lax.all_to_all(ordered, "dp", split_axis=0, concat_axis=0, tiled=True)
        )
    served = None
    for span, owned in zip(kind_spans, arrived):
        served = join_strips(owned, strip_width, span.start, served)

    squares = jnp.sum(sums[:, 0, 0])
    clip_factor = jnp.minimum(1.0, lax.rsqrt(squares / entries + norm_eps))
    new_master, new_one, new_two = adam_update(
        master, moment_one, moment_two, gradients, clip_factor
    )
    parts = expert_parts(blocks, weight_sets, hidden_total)
    for place, offsets in enumerate(stages):
        summed = parts[0]
        for index, k in reversed(list(enumerate(offsets[1:], 1))):
            summed = summed + exchange(parts[index], k, member_count).astype(jnp.float32)
        if place < len(stages) - 1:
            extent = summed.shape[0] // len(offsets)
            pieces = [summed[i * extent : (i + 1) * extent] for i in range(len(offsets))]
            parts = pieces[:1] + [piece.astype(jnp.bfloat16) for piece in pieces[1:]]
    decoded = hidden_in.astype(jnp.float32) + summed.reshape(hidden_in.shape)
    return (new_master, new_one, new_two, served, decoded.astype(jnp.bfloat16))


def solution(mesh):
    in_specs = (
        P(None, None, "dp", "tensor"),
        P(None, None, "dp", "tensor"),
        P(None, None, "dp", "tensor"),
        P(None, None, "dp", "tensor"),
        P(),
        P(None, ("dp", "tensor"), None),
        P(None, ("dp", "tensor"), None),
        P(None, ("dp", "tensor"), None),
    )
    out_specs = (
        P(None, None, "dp", "tensor"),
        P(None, None, "dp", "tensor"),
        P(None, None, "dp", "tensor"),
        P(None, "dp", None),
        P(None, ("dp", "tensor"), None),
    )

    return jax.shard_map(
        per_device, mesh=mesh, in_specs=in_specs, out_specs=out_specs, check_vma=False
    )
```
